32 devices in a mesh: gx: 4 (over x, core), gy: 2 (over y), gz: 4 (over z).
Axes of the slice: x: 2, y: 2, z: 4, core: 2. Of those that a mesh axis runs over, the one named last changes fastest.
Arguments:
- right_side: float32 [32, 32, 512], P('gx', 'gy', 'gz'), may hold values from -6 to 6
- conductance: float32 [32, 32, 512], P('gx', 'gy', 'gz'), may hold values from 0.25 to 4
- extents: int32 [4, 2, 4], P('gx', 'gy', 'gz'), may hold values from 64 to 128, as said below
- coarse_factor: bfloat16 [32, 32], replicated, may hold values from -1 to 3, as said below
Outputs:
- solution_field: float32 [32, 32, 512], P('gx', 'gy', 'gz')
- residual: float32 [32, 32, 512], P('gx', 'gy', 'gz')
The draws below stay inside these ranges and needn't reach their ends.
Inputs may be any that keep to these rules, and one draw needn't show every extreme that they name: `extents`: cells of a block whose third local index is below its count are fluid, the others padding; in every draw some block has all 128 layers fluid. `coarse_factor`: lower triangular with a positive diagonal.
All inputs are finite; a program needn't handle non-finite values.
Results may differ from the reference program's by a relative error of at most 0.0003.
Values sent between devices are 32-bit elements; how exact they have to be, the bound alone decides.
A program may use at most 64 MiB of HBM per device.

```python
import math
import jax
import jax.numpy as jnp
from jax import lax

CX = 8
CY = 16
CZ = 128
ITERS = 2
NX = 32
NY = 32
NZ = 512
NB = 32
N_GX = 4
N_GY = 2
N_GZ = 4


def draw_right_side(key, part):
    key_cells, key_blocks = jax.random.split(jax.random.fold_in(key, 11), 2)
    blocks = (NX // CX, NY // CY, NZ // CZ)
    values = jnp.clip(jax.random.normal(key_cells, (NX, NY, NZ), jnp.float32), -4.0, 4.0)
    offsets = jax.random.uniform(key_blocks, blocks, jnp.float32, -1.5, 1.5)
    spread = jnp.repeat(jnp.repeat(jnp.repeat(offsets, CX, axis=0), CY, axis=1), CZ, axis=2)
    return values + spread


def draw_extents(key, part):
    key_counts, key_full = jax.random.split(jax.random.fold_in(key, 23))
    blocks = (NX // CX, NY // CY, NZ // CZ)
    counts = jax.random.randint(key_counts, blocks, CZ // 2, CZ + 1).reshape(-1)
    chosen = jax.random.randint(key_full, (), 0, counts.shape[0])
    counts = jnp.where(jnp.arange(counts.shape[0]) == chosen, CZ, counts)
    return counts.reshape(blocks).astype(jnp.int32)


def draw_coarse_factor(key, part):
    key_diag, key_low = jax.random.split(jax.random.fold_in(key, 37))
    diagonal = jax.random.uniform(key_diag, (NB,), jnp.float32, 1.0, 2.0)
    lower = jnp.clip(jax.random.normal(key_low, (NB, NB), jnp.float32), -6.0, 6.0)
    lower = jnp.tril(lower, -1) * (0.5 / math.sqrt(NB))
    return (lower + jnp.diag(diagonal)).astype(jnp.bfloat16)


def shard_levels(rng, shape, cuts, low, top_value):
    def one(axis_at, shards_of):
        steps = jax.random.uniform(jax.random.fold_in(jax.random.fold_in(rng, 6), axis_at), (shards_of,), jnp.float32, low / len(cuts), top_value / len(cuts))
        return jnp.repeat(jnp.exp(steps), shape[axis_at] // shards_of).reshape((-1,) + (1,) * (len(shape) - axis_at - 1))

    loudness = one(*cuts[0])
    for cut in cuts[1:]:
        loudness = loudness * one(*cut)
    return loudness


def setup_inputs(seed: int = 0) -> dict:
    streams_of = jax.random.split(jax.random.key(seed), 5)
    right_side = draw_right_side(jax.random.fold_in(streams_of[4], 71), 0)
    conductance = jnp.clip(jnp.exp(math.log(4.0) - 2.7725887 * jax.random.uniform(streams_of[1], (NX, NY, NZ), jnp.float32) ** shard_levels(streams_of[1], (NX, NY, NZ), ((0, 4), (1, 2), (2, 4)), -0.2, 0.2)), 0.25, 4.0)
    extents = draw_extents(jax.random.fold_in(streams_of[4], 71), 0)
    coarse_factor = draw_coarse_factor(jax.random.fold_in(streams_of[4], 71), 0)
    return dict(right_side=right_side, conductance=conductance, extents=extents, coarse_factor=coarse_factor)


OMEGA = 0.8

def neighbour_slices():
    inner = slice(1, -1)
    return [(slice(2, None), inner, inner), (slice(None, -2), inner, inner), (inner, slice(2, None), inner), (inner, slice(None, -2), inner), (inner, inner, slice(2, None)), (inner, inner, slice(None, -2))]

def face_terms(padded, cond_padded):
    centre = (slice(1, -1), slice(1, -1), slice(1, -1))
    value_mid = padded[centre]
    cond_mid = cond_padded[centre]
    summed = jnp.zeros_like(value_mid)
    for place in neighbour_slices():
        summed = summed + 0.5 * (cond_mid + cond_padded[place]) * (value_mid - padded[place])
    return summed

def coef_total(cond_padded):
    centre = (slice(1, -1), slice(1, -1), slice(1, -1))
    cond_mid = cond_padded[centre]
    summed = jnp.zeros_like(cond_mid)
    for place in neighbour_slices():
        summed = summed + 0.5 * (cond_mid + cond_padded[place])
    return summed

def pool_sum(field):
    first, second, third = field.shape
    return field.reshape(first // 2, 2, second // 2, 2, third // 2, 2).sum(axis=(1, 3, 5))

def pool_max(field):
    first, second, third = field.shape
    return field.reshape(first // 2, 2, second // 2, 2, third // 2, 2).max(axis=(1, 3, 5))

def expand(field):
    first, second, third = field.shape
    wide = jnp.broadcast_to(field[:, None, :, None, :, None], (first, 2, second, 2, third, 2))
    return wide.reshape(2 * first, 2 * second, 2 * third)

def make_level(cond_padded, fluid, scale):
    inverse = fluid / (scale * coef_total(cond_padded) + 1.0 - fluid)
    return (cond_padded, fluid, scale, inverse)

def apply_level(field, level):
    padded = jnp.pad(field, 1)
    return level[2] * level[1] * face_terms(padded, level[0])

def cycle(resid, levels, depth):
    level = levels[depth]
    first = OMEGA * level[3] * resid
    if depth == len(levels) - 1:
        return first
    image = apply_level(first, level)
    below = cycle(pool_sum(resid - image), levels, depth + 1)
    second = first + level[1] * expand(below)
    return second + OMEGA * level[3] * (resid - apply_level(second, level))

def reference(right_side, conductance, extents, coarse_factor):
    factor = coarse_factor.astype(jnp.float32)
    layer = lax.broadcasted_iota(jnp.int32, right_side.shape, 2) % CZ
    limit = jnp.repeat(jnp.repeat(jnp.repeat(extents, CX, axis=0), CY, axis=1), CZ, axis=2)
    fluid = (layer < limit).astype(jnp.float32)
    fluid_mid = pool_max(fluid)
    cond_mid = pool_sum(conductance) / 8.0
    levels = [make_level(jnp.pad(conductance, 1), fluid, 1.0), make_level(jnp.pad(cond_mid, 1), fluid_mid, 4.0)]
    block_cells = CX * CY * CZ

    def precondition(resid):
        smoothed = cycle(resid, levels, 0)
        means = resid.reshape(N_GX, CX, N_GY, CY, N_GZ, CZ).sum(axis=(1, 3, 5)).reshape(-1) / block_cells
        coarse = jax.scipy.linalg.cho_solve((factor, True), means)
        blockwise = coarse.reshape(N_GX, N_GY, N_GZ)
        spread = jnp.repeat(jnp.repeat(jnp.repeat(blockwise, CX, axis=0), CY, axis=1), CZ, axis=2)
        return smoothed + fluid * spread
    resid = fluid * right_side
    solution = jnp.zeros_like(resid)
    precond = precondition(resid)
    inner_now = jnp.sum(resid * precond)
    direction = precond
    for step in range(ITERS):
        image = apply_level(direction, levels[0])
        alpha = inner_now / jnp.sum(direction * image)
        solution = solution + alpha * direction
        resid = resid - alpha * image
        if step + 1 < ITERS:
            precond = precondition(resid)
            inner_next = jnp.sum(resid * precond)
            direction = precond + inner_next / inner_now * direction
            inner_now = inner_next
    return (solution, resid)
```

```python
import functools

import jax
import jax.numpy as jnp
from jax import lax
from jax.experimental import pallas as pl
from jax.experimental.pallas import tpu as pltpu
from jax.sharding import PartitionSpec as P

OMEGA = 0.8
HALO = 4
MESH = pl.DeviceIdType.MESH
HIGH = lax.Precision.HIGHEST
DIRS = [
    (dx, dy, dz)
    for dx in (-1, 0, 1)
    for dy in (-1, 0, 1)
    for dz in (-1, 0, 1)
    if (dx, dy, dz) != (0, 0, 0)
]


def code(dx, dy, dz):
    return (dx + 1) * 9 + (dy + 1) * 3 + dz + 1


def kernel(
    counts,
    rhs_ref,
    cond_ref,
    ext_ref,
    factor_ref,
    sol_ref,
    res_ref,
    h_out,
    p_out,
    e_out,
    x_in,
    h_in,
    p_in,
    e_in,
    av_out,
    h2_out,
    p2_out,
    x2_in,
    h2_in,
    p2_in,
    row_out,
    row2_out,
    gath,
    gath2,
    R,
    C,
    FL,
    FX,
    FY,
    FZ,
    INV,
    C1,
    IC,
    FIRST,
    SEC,
    V,
    U,
    YT,
    D0,
    AD0,
    AV1,
    send_a,
    recv_a,
    send_e,
    recv_e,
    send_b,
    recv_b,
    send_g,
    recv_g,
):
    ngx, ngy, ngz = counts
    n = ngx * ngy * ngz
    ix, iy, iz = lax.axis_index("gx"), lax.axis_index("gy"), lax.axis_index("gz")
    me = (ix * ngy + iy) * ngz + iz
    bx, by, bz = rhs_ref.shape
    ex, ey, ez = bx + 2 * HALO, by + 2 * HALO, 2 * bz
    group = 2 * HALO
    half = bz // 2
    f32 = jnp.float32

    def coords(flat):
        return (flat // (ngy * ngz), (flat // ngz) % ngy, flat % ngz)

    barrier = pltpu.get_barrier_semaphore()

    def greet(t, carry):
        pl.semaphore_signal(
            barrier, inc=1, device_id=coords((me + t) % n), device_id_type=MESH
        )
        return carry

    for buf in (x_in, h_in, p_in, e_in, x2_in, h2_in, p2_in):
        buf[...] = jnp.zeros(buf.shape, f32)
    lax.fori_loop(1, n, greet, 0)

    lane = lax.broadcasted_iota(jnp.int32, (ey, bz), 1)
    row8 = lax.broadcasted_iota(jnp.int32, (2 * HALO, bz), 0)

    def edge_tile(slab):
        return jnp.where(row8 < HALO, slab[: 2 * HALO], slab[by - 2 * HALO :])

    def pack(slabs):
        packed = jnp.zeros((ey, bz), f32)
        for at, (slab, tile) in enumerate(slabs):
            full = jnp.concatenate([slab, tile], axis=0)
            moved = pltpu.roll(full, (HALO + group * at) % bz, 1)
            packed = jnp.where(lane // group == at, moved, packed)
        return packed

    slabs = []
    for f, ref in enumerate((rhs_ref, cond_ref)):
        for x in range(bx):
            slab = ref[x]
            tile = edge_tile(slab)
            h_out[f, x] = tile
            slabs.append((slab, tile))
    p_out[...] = pack(slabs)
    own_limit = ext_ref[0, 0, 0]
    e_out[...] = jnp.full((1, bz), own_limit.astype(f32), f32)

    L = factor_ref[...].astype(f32)
    ri = lax.broadcasted_iota(jnp.int32, (n, n), 0)
    ci = lax.broadcasted_iota(jnp.int32, (n, n), 1)
    eye = ri == ci
    X = jnp.where(eye, 1.0 / jnp.where(eye, L, 1.0), 0.0)
    s = 1
    while s < n:
        pick = (ri // (2 * s) == ci // (2 * s)) & (ri % (2 * s) >= s) & (ci % (2 * s) < s)
        low = jnp.where(pick, L, 0.0)
        X = X - jnp.dot(
            X,
            jnp.dot(low, X, precision=HIGH, preferred_element_type=f32),
            precision=HIGH,
            preferred_element_type=f32,
        )
        s *= 2
    W = lax.dot_general(
        X, X, (((0,), (0,)), ((), ())), precision=HIGH, preferred_element_type=f32
    )

    pl.semaphore_wait(barrier, n - 1)

    def inside(d):
        dx, dy, dz = d
        ok = None
        for at, step, count in ((ix, dx, ngx), (iy, dy, ngy), (iz, dz, ngz)):
            if step == 0:
                continue
            here = (at + step >= 0) & (at + step < count)
            ok = here if ok is None else ok & here
        return ok

    def target(d):
        return (ix + d[0], iy + d[1], iz + d[2])

    def remote(src, dst, send, recv, d):
        return pltpu.make_async_remote_copy(
            src_ref=src,
            dst_ref=dst,
            send_sem=send,
            recv_sem=recv,
            device_id=target(d),
            device_id_type=MESH,
        )

    def x_part(dx):
        if dx == 0:
            return pl.ds(0, bx), pl.ds(HALO, bx)
        if dx == 1:
            return pl.ds(bx - HALO, HALO), pl.ds(0, HALO)
        return pl.ds(0, HALO), pl.ds(bx + HALO, HALO)

    def side(dx):
        return 0 if dx == 1 else 1

    def copies_a(d):
        dx, dy, dz = d
        k = code(*d)
        out = [remote(e_out, e_in.at[code(-dx, -dy, -dz)], send_e.at[k], recv_e.at[k], d)]
        if dz != 0:
            slot = code(-dx, -dy, -dz)
            out.append(remote(p_out, p_in.at[slot], send_a.at[k, 0], recv_a.at[k, 0], d))
        elif dy != 0:
            src, dst = x_part(dx)
            out.append(
                remote(
                    h_out.at[:, src],
                    h_in.at[side(dy), :, dst],
                    send_a.at[k, 0],
                    recv_a.at[k, 0],
                    d,
                )
            )
        else:
            src, _ = x_part(dx)
            for f, ref in enumerate((rhs_ref, cond_ref)):
                out.append(
                    remote(
                        ref.at[src],
                        x_in.at[side(dx), f],
                        send_a.at[k, f],
                        recv_a.at[k, f],
                        d,
                    )
                )
        return out

    def copies_b(d):
        dx, dy, dz = d
        k = code(*d)
        if dz != 0:
            slot = code(-dx, -dy, -dz)
            return [remote(p2_out, p2_in.at[slot], send_b.at[k], recv_b.at[k], d)]
        src, dst = x_part(dx)
        if dy != 0:
            return [
                remote(
                    h2_out.at[src], h2_in.at[side(dy), dst], send_b.at[k], recv_b.at[k], d
                )
            ]
        return [remote(av_out.at[src], x2_in.at[side(dx)], send_b.at[k], recv_b.at[k], d)]

    def start_all(copies):
        for d in DIRS:

            @pl.when(inside(d))
            def _():
                for c in copies(d):
                    c.start()

    def wait_all(copies):
        for d in DIRS:
            @pl.when(inside(tuple(-a for a in d)))
            def _():
                for c in copies(d):
                    c.wait_recv()

        for d in DIRS:

            @pl.when(inside(d))
            def _():
                for c in copies(d):
                    c.wait_send()

    start_all(copies_a)

    rowe = lax.broadcasted_iota(jnp.int32, (ey, bz), 0)
    low_lanes = (lane % group) < HALO

    def merge_h(h, *at):
        return jnp.where(row8 < HALO, h[(1,) + at], h[(0,) + at])

    def merge_p(p):
        merged = []
        for dx in (-1, 0, 1):

            def from_z(dy):
                return jnp.where(
                    low_lanes, p[code(dx, dy, 1)], p[code(dx, dy, -1)]
                ), jnp.where(low_lanes, p[code(dx, dy, -1)], p[code(dx, dy, 1)])

            mid = from_z(0)[1]
            up = from_z(1)[1]
            down = from_z(-1)[1]
            merged.append(
                jnp.where(rowe < by, mid, jnp.where(rowe < by + HALO, up, down))
            )
        return merged

    def where_from(x):
        if x < HALO:
            return 0, bx - HALO + x
        if x < HALO + bx:
            return 1, x - HALO
        return 2, x - HALO - bx

    def unpack(merged, x, f):
        which, slab = where_from(x)
        at = f * bx + slab
        return pltpu.roll(merged[which], (bz - HALO - group * at) % bz, 1)

    wait_all(copies_a)

    merged = merge_p(p_in)
    limits = []
    for dx in (-1, 0, 1):
        sides = []
        for dz in (0, 1, -1):

            def limit(dy):
                if (dx, dy, dz) == (0, 0, 0):
                    return e_out[...]
                return e_in[code(dx, dy, dz)]

            sides.append(
                jnp.where(rowe < by, limit(0), jnp.where(rowe < by + HALO, limit(1), limit(-1)))
            )
        limits.append((sides[0], jnp.where(lane < half, sides[1], sides[2])))
    flags, flags1 = [], []
    lane_f = lane.astype(f32)
    even_f = (lane - lane % 2).astype(f32)
    for a, b in limits:
        flags.append(
            jnp.concatenate([(lane_f < a).astype(f32), (lane_f < b).astype(f32)], axis=1)
        )
        flags1.append(
            jnp.concatenate([(even_f < a).astype(f32), (even_f < b).astype(f32)], axis=1)
        )
    for x in range(ex):
        which, _ = where_from(x)
        FL[x] = flags[which]
        for f, (ref, field) in enumerate(((rhs_ref, R), (cond_ref, C))):
            if which == 1:
                core = ref[x - HALO]
            elif which == 0:
                core = x_in[0, f, x]
            else:
                core = x_in[1, f, x - HALO - bx]
            a = jnp.concatenate([core, merge_h(h_in, f, x)], axis=0)
            whole = jnp.concatenate([a, unpack(merged, x, f)], axis=1)
            field[x] = whole * flags[which] if f == 0 else whole

    wide_lane = lax.broadcasted_iota(jnp.int32, (ey, ez), 1)
    wide_row = lax.broadcasted_iota(jnp.int32, (ey, ez), 0)
    odd_lane = wide_lane % 2 == 1
    odd_row = wide_row % 2 == 1

    def up_y(v, k=1):
        return pltpu.roll(v, k, 0)

    def dn_y(v, k=1):
        return pltpu.roll(v, ey - k, 0)

    def up_z(v, k=1):
        return pltpu.roll(v, k, 1)

    def dn_z(v, k=1):
        return pltpu.roll(v, ez - k, 1)

    def pool_yz(v):
        v = v + jnp.where(odd_row, up_y(v), dn_y(v))
        return v + jnp.where(odd_lane, up_z(v), dn_z(v))

    for x in range(ex):
        c = C[x]
        if x > 0:
            FX[x] = 0.5 * (C[x - 1] + c)
        FY[x] = 0.5 * (c + up_y(c))
        FZ[x] = 0.5 * (c + up_z(c))
    for x in range(1, ex - 1):
        fy, fz = FY[x], FZ[x]
        total = FX[x] + FX[x + 1] + fy + dn_y(fy) + fz + dn_z(fz)
        fl = FL[x]
        INV[x] = OMEGA * fl / (total + 1.0 - fl)
    for q in range(ex // 2):
        C1[q] = pool_yz(C[2 * q] + C[2 * q + 1]) * 0.125
    for q in range(1, ex // 2 - 1):
        c = C1[q]
        total = 3.0 * c + 0.5 * (
            C1[q - 1] + C1[q + 1] + up_y(c, 2) + dn_y(c, 2) + up_z(c, 2) + dn_z(c, 2)
        )
        fl = flags1[where_from(2 * q)[0]]
        IC[q] = OMEGA * fl / (4.0 * total + 1.0 - fl)

    def apply(src, x):
        v = src[x]
        gx = FX[x] * (v - src[x - 1]) + FX[x + 1] * (v - src[x + 1])
        gy = FY[x] * (v - up_y(v))
        gz = FZ[x] * (v - up_z(v))
        return FL[x] * (gx + (gy - dn_y(gy)) + (gz - dn_z(gz)))

    def core(v):
        return v[:by, :bz]

    def cycle():
        for x in range(1, ex - 1):
            FIRST[x] = INV[x] * R[x]
        for q in range(1, ex // 2 - 1):
            a, b = 2 * q, 2 * q + 1
            gap = (R[a] - apply(FIRST, a)) + (R[b] - apply(FIRST, b))
            below = IC[q] * pool_yz(gap)
            SEC[a] = FIRST[a] + FL[a] * below
            SEC[b] = FIRST[b] + FL[b] * below
        for x in range(3, ex - 3):
            V[x] = SEC[x] + INV[x] * (R[x] - apply(SEC, x))

    def total(v):
        return jnp.sum(v, axis=(0, 1), keepdims=True)

    width = gath.shape[-1]
    col = lax.broadcasted_iota(jnp.int32, (1, width), 1)

    def spread(row_ref, g, base):
        def send(t, carry):
            remote_row(row_ref, g, base, (me + t) % n).start()
            return carry

        lax.fori_loop(1, n, send, 0)

    def remote_row(row_ref, g, base, flat):
        return pltpu.make_async_remote_copy(
            src_ref=row_ref,
            dst_ref=g.at[me],
            send_sem=send_g.at[base],
            recv_sem=recv_g.at[base],
            device_id=coords(flat),
            device_id_type=MESH,
        )

    def collect(g, base):
        part = g.at[pl.ds(0, n - 1)]
        pltpu.make_async_copy(part, part, recv_g.at[base]).wait()
        pltpu.make_async_copy(part, part, send_g.at[base]).wait()

    cells = bx * by * bz

    cycle()
    sums = [jnp.zeros((by, bz), f32) for _ in range(4)]
    slabs = []
    for x in range(bx):
        e = x + HALO
        av = core(apply(V, e))
        v, r = core(V[e]), core(R[e])
        av_out[x] = av
        tile = edge_tile(av)
        h2_out[x] = tile
        slabs.append((av, tile))
        sums = [sums[0] + r, sums[1] + r * v, sums[2] + v * av, sums[3] + av]
    p2_out[...] = pack(slabs)
    start_all(copies_b)

    acc = jnp.zeros((by, bz), f32)
    for x in range(HALO, HALO + bx):
        acc = acc + core(apply(FL, x))
    faces = []
    for dx, x, near in ((-1, HALO, HALO - 1), (1, HALO + bx, HALO + bx - 1)):
        other = FL[x] if dx == 1 else FL[near]
        mine = FL[near] if dx == 1 else FL[x]
        faces.append(((dx, 0, 0), total(core(FX[x] * mine * other))))
    first_row = wide_row[:by, :bz] == 0
    last_row = wide_row[:by, :bz] == by - 1
    first_lane = wide_lane[:by, :bz] == 0
    last_lane = wide_lane[:by, :bz] == bz - 1
    cy = jnp.zeros((ey, ez), f32)
    cz = jnp.zeros((ey, ez), f32)
    for x in range(HALO, HALO + bx):
        fl = FL[x]
        cy = cy + FY[x] * fl * up_y(fl)
        cz = cz + FZ[x] * fl * up_z(fl)
    cy_hi, cz_hi = core(dn_y(cy)), core(dn_z(cz))
    faces.append(((0, -1, 0), total(jnp.where(first_row, core(cy), 0.0))))
    faces.append(((0, 1, 0), total(jnp.where(last_row, cy_hi, 0.0))))
    faces.append(((0, 0, -1), total(jnp.where(first_lane, core(cz), 0.0))))
    faces.append(((0, 0, 1), total(jnp.where(last_lane, cz_hi, 0.0))))
    diagonal = total(acc)
    row = jnp.zeros((1, width), f32)
    for (dx, dy, dz), g in faces:
        diagonal = diagonal + g
        other = ((ix + dx) * ngy + iy + dy) * ngz + iz + dz
        row = row - jnp.where(col == bz + other, g, 0.0)
    row = row + jnp.where(col == bz + me, diagonal, 0.0)
    for k, part in enumerate(sums):
        row = jnp.where(col == k, total(part), row)
    row_out[...] = row
    gath[pl.ds(me, 1)] = row[None]
    spread(row_out, gath, 0)
    collect(gath, 0)

    def column(g, k):
        return g[:, 0, k : k + 1]

    def solve(means_col):
        y_row = jnp.sum(W * means_col, axis=0, keepdims=True)
        y_col = jnp.sum(jnp.where(eye, y_row, 0.0), axis=1, keepdims=True)
        return y_row, y_col

    ycol_id = lax.broadcasted_iota(jnp.int32, (ey, n), 1)
    yrow_id = lax.broadcasted_iota(jnp.int32, (ey, n), 0)
    dy_id = jnp.where(yrow_id < by, 0, jnp.where(yrow_id < by + HALO, 1, -1))

    def make_table(y_row):
        for dx in (-1, 0, 1):
            cols = []
            for dz in (0, 1, -1):
                where_at = ((ix + dx) * ngy + iy + dy_id) * ngz + iz + dz
                cols.append(
                    jnp.sum(jnp.where(ycol_id == where_at, y_row, 0.0), axis=1, keepdims=True)
                )
            YT[dx + 1] = jnp.concatenate(
                [
                    jnp.broadcast_to(cols[0], (ey, bz)),
                    jnp.where(lane < half, cols[1], cols[2]),
                ],
                axis=1,
            )

    coupling = gath[:, 0, bz : bz + n]
    m0 = column(gath, 0)
    y_row, y_col = solve(m0 * (1.0 / cells))
    rz = total(column(gath, 1)) + total(m0 * y_col)
    dad = (
        total(column(gath, 2))
        + 2.0 * total(column(gath, 3) * y_col)
        + total(coupling * y_col * y_row)
    )
    alpha = rz / dad
    make_table(y_row)
    for x in range(ex):
        U[x] = FL[x] * YT[where_from(x)[0]]

    wait_all(copies_b)
    merged = merge_p(p2_in)
    for x in range(1, ex - 1):
        which, _ = where_from(x)
        au = apply(U, x)
        if which == 1:
            mid = av_out[x - HALO]
        elif which == 0:
            mid = x2_in[0, x]
        else:
            mid = x2_in[1, x - HALO - bx]
        a = jnp.concatenate([mid, merge_h(h2_in, x)], axis=0)
        ad = jnp.concatenate([a, unpack(merged, x, 0)], axis=1) + au
        R[x] = R[x] - alpha * ad
        if which == 1:
            AD0[x - HALO] = core(ad)
            D0[x - HALO] = core(V[x]) + core(U[x])

    cycle()
    sums = [jnp.zeros((by, bz), f32) for _ in range(6)]
    for x in range(bx):
        e = x + HALO
        av = core(apply(V, e))
        v, r, ad0 = core(V[e]), core(R[e]), AD0[x]
        AV1[x] = av
        sums = [
            sums[0] + r,
            sums[1] + r * v,
            sums[2] + v * av,
            sums[3] + av,
            sums[4] + v * ad0,
            sums[5] + ad0,
        ]
    row = jnp.zeros((1, bz), f32)
    for k, part in enumerate(sums):
        row = jnp.where(col[:, :bz] == k, total(part), row)
    row2_out[...] = row
    gath2[pl.ds(me, 1)] = row[None]
    spread(row2_out, gath2, 1)
    collect(gath2, 1)
    m1 = column(gath2, 0)
    y_row, y_col = solve(m1 * (1.0 / cells))
    new = total(column(gath2, 1)) + total(m1 * y_col)
    beta = new / rz
    dad1 = (
        total(column(gath2, 2))
        + 2.0 * total(column(gath2, 3) * y_col)
        + total(coupling * y_col * y_row)
        + 2.0 * beta * (total(column(gath2, 4)) + total(column(gath2, 5) * y_col))
        + beta * beta * dad
    )
    alpha1 = new / dad1
    make_table(y_row)
    for x in range(HALO - 1, HALO + bx + 1):
        U[x] = FL[x] * YT[where_from(x)[0]]
    for x in range(bx):
        e = x + HALO
        d1 = core(V[e]) + core(U[e]) + beta * D0[x]
        ad1 = AV1[x] + core(apply(U, e)) + beta * AD0[x]
        sol_ref[x] = alpha * D0[x] + alpha1 * d1
        res_ref[x] = core(R[e]) - alpha1 * ad1


def solution(mesh):
    counts = (mesh.shape["gx"], mesh.shape["gy"], mesh.shape["gz"])
    n = counts[0] * counts[1] * counts[2]

    def on_device(right_side, conductance, extents, coarse_factor):
        f32 = jnp.float32
        bx, by, bz = right_side.shape
        ex, ey, ez = bx + 2 * HALO, by + 2 * HALO, 2 * bz
        tall = 2 * HALO
        width = bz + -(-n // 128) * 128
        vm = lambda *shape: pltpu.VMEM(shape, f32)
        field = vm(ex, ey, ez)
        dma = pltpu.SemaphoreType.DMA
        scratch = [
            vm(2, bx, tall, bz),
            vm(ey, bz),
            vm(1, bz),
            vm(2, 2, HALO, by, bz),
            vm(2, 2, ex, tall, bz),
            vm(27, ey, bz),
            vm(27, 1, bz),
            vm(bx, by, bz),
            vm(bx, tall, bz),
            vm(ey, bz),
            vm(2, HALO, by, bz),
            vm(2, ex, tall, bz),
            vm(27, ey, bz),
            vm(1, width),
            vm(1, bz),
            vm(n, 1, width),
            vm(n, 1, bz),
            field,
            field,
            field,
            field,
            field,
            field,
            field,
            vm(ex // 2, ey, ez),
            vm(ex // 2, ey, ez),
            field,
            field,
            field,
            field,
            vm(3, ey, ez),
            vm(bx, by, bz),
            vm(bx, by, bz),
            vm(bx, by, bz),
            dma((27, 2)),
            dma((27, 2)),
            dma((27,)),
            dma((27,)),
            dma((27,)),
            dma((27,)),
            dma((2,)),
            dma((2,)),
        ]
        block = jax.ShapeDtypeStruct((bx, by, bz), f32)
        whole = pl.BlockSpec(memory_space=pltpu.VMEM)
        return pl.pallas_call(
            functools.partial(kernel, counts),
            out_shape=(block, block),
            in_specs=[whole, whole, pl.BlockSpec(memory_space=pltpu.SMEM), whole],
            out_specs=(whole, whole),
            scratch_shapes=scratch,
            compiler_params=pltpu.CompilerParams(
                collective_id=0, has_side_effects=True, vmem_limit_bytes=48 * 1024 * 1024
            ),
        )(right_side, conductance, extents, coarse_factor)

    in_specs = (P("gx", "gy", "gz"), P("gx", "gy", "gz"), P("gx", "gy", "gz"), P())
    out_specs = (P("gx", "gy", "gz"), P("gx", "gy", "gz"))
    return jax.shard_map(
        on_device, mesh=mesh, in_specs=in_specs, out_specs=out_specs, check_vma=False
    )
```

```python
import functools

import jax
import jax.numpy as jnp
from jax import lax
from jax.experimental import pallas as pl
from jax.experimental.pallas import tpu as pltpu
from jax.sharding import PartitionSpec as P

OMEGA = 0.8
HALO = 4
MESH = pl.DeviceIdType.MESH
HIGH = lax.Precision.HIGHEST
DIRS = [
    (dx, dy, dz)
    for dx in (-1, 0, 1)
    for dy in (-1, 0, 1)
    for dz in (-1, 0, 1)
    if (dx, dy, dz) != (0, 0, 0)
]
DIRS.sort(key=lambda d: -sum(abs(a) for a in d))


def code(dx, dy, dz):
    return (dx + 1) * 9 + (dy + 1) * 3 + dz + 1


def kernel(
    counts,
    rhs_hbm,
    cond_hbm,
    ext_ref,
    factor_hbm,
    sol_ref,
    res_ref,
    rhs_ref,
    cond_ref,
    factor_ref,
    h_out,
    p_out,
    e_out,
    x_in,
    h_in,
    p_in,
    e_in,
    av_out,
    h2_out,
    p2_out,
    x2_in,
    h2_in,
    p2_in,
    row_out,
    row2_out,
    gath,
    gath2,
    R,
    C,
    FL,
    FX,
    FY,
    FZ,
    INV,
    C1,
    IC,
    FIRST,
    SEC,
    V,
    U,
    YT,
    D0,
    AD0,
    AV1,
    send_a,
    recv_a,
    send_e,
    recv_e,
    send_b,
    recv_b,
    send_g,
    recv_g,
    load_sem,
):
    ngx, ngy, ngz = counts
    n = ngx * ngy * ngz
    ix, iy, iz = lax.axis_index("gx"), lax.axis_index("gy"), lax.axis_index("gz")
    me = (ix * ngy + iy) * ngz + iz
    bx, by, bz = rhs_ref.shape
    ex, ey, ez = bx + 2 * HALO, by + 2 * HALO, 2 * bz
    group = 2 * HALO
    half = bz // 2
    f32 = jnp.float32

    loads = [
        pltpu.make_async_copy(src, dst, load_sem.at[k])
        for k, (src, dst) in enumerate(
            ((rhs_hbm, rhs_ref), (cond_hbm, cond_ref), (factor_hbm, factor_ref))
        )
    ]
    for load in loads:
        load.start()

    def turned(at, step, count):
        moved = at + step
        return jnp.where(moved >= count, moved - count, moved)

    def everyone(act):
        if n <= 64:
            xs = [turned(ix, t, ngx) for t in range(ngx)]
            ys = [turned(iy, t, ngy) for t in range(ngy)]
            zs = [turned(iz, t, ngz) for t in range(ngz)]
            steps = [(a, b, c) for a in range(ngx) for b in range(ngy) for c in range(ngz)]
            steps.sort(
                key=lambda t: -sum(min(a, m - a) for a, m in zip(t, (ngx, ngy, ngz)))
            )
            for a, b, c in steps[:-1]:
                act((xs[a], ys[b], zs[c]))
        else:

            def one(t, carry):
                flat = (me + t) % n
                act((flat // (ngy * ngz), (flat // ngz) % ngy, flat % ngz))
                return carry

            lax.fori_loop(1, n, one, 0)

    for buf in (x_in, h_in, p_in, e_in, x2_in, h2_in, p2_in):
        buf[...] = jnp.zeros(buf.shape, f32)

    barrier = pltpu.get_barrier_semaphore()
    everyone(
        lambda device: pl.semaphore_signal(
            barrier, inc=1, device_id=device, device_id_type=MESH
        )
    )

    lane = lax.broadcasted_iota(jnp.int32, (ey, bz), 1)
    row8 = lax.broadcasted_iota(jnp.int32, (2 * HALO, bz), 0)

    def edge_tile(slab):
        return jnp.where(row8 < HALO, slab[: 2 * HALO], slab[by - 2 * HALO :])

    def pack_pairs(out, lows, highs):
        for p in range(len(lows) // 2):
            out[0][p] = jnp.where(
                row8 < HALO, pltpu.roll(highs[2 * p], HALO, 0), highs[2 * p + 1]
            )
            out[1][p] = jnp.where(
                row8 < HALO, lows[2 * p], pltpu.roll(lows[2 * p + 1], HALO, 0)
            )

    def pack(slabs):
        packed = jnp.zeros((ey, bz), f32)
        for at, (slab, tile) in enumerate(slabs):
            full = jnp.concatenate([slab, tile], axis=0)
            moved = pltpu.roll(full, (HALO + group * at) % bz, 1)
            packed = jnp.where(lane // group == at, moved, packed)
        return packed

    for load in loads[:2]:
        load.wait()
    tall = 2 * HALO
    slabs = []
    for f, ref in enumerate((rhs_ref, cond_ref)):
        fields = [ref[x] for x in range(bx)]
        pack_pairs(
            (h_out.at[0, f], h_out.at[1, f]),
            [v[:tall] for v in fields],
            [v[by - tall :] for v in fields],
        )
        slabs.extend((v, edge_tile(v)) for v in fields)
    p_out[...] = pack(slabs)
    own_limit = ext_ref[0, 0, 0]
    e_out[...] = jnp.full((1, bz), own_limit.astype(f32), f32)

    pl.semaphore_wait(barrier, n - 1)

    def inside(d):
        dx, dy, dz = d
        ok = None
        for at, step, count in ((ix, dx, ngx), (iy, dy, ngy), (iz, dz, ngz)):
            if step == 0:
                continue
            here = (at + step >= 0) & (at + step < count)
            ok = here if ok is None else ok & here
        return ok

    def target(d):
        return (ix + d[0], iy + d[1], iz + d[2])

    def remote(src, dst, send, recv, d):
        return pltpu.make_async_remote_copy(
            src_ref=src,
            dst_ref=dst,
            send_sem=send,
            recv_sem=recv,
            device_id=target(d),
            device_id_type=MESH,
        )

    def x_part(dx):
        return pl.ds(bx - HALO, HALO) if dx == 1 else pl.ds(0, HALO)

    def pair_part(dx):
        few, all_ = HALO // 2, bx // 2
        if dx == 0:
            return pl.ds(0, all_), pl.ds(few, all_)
        if dx == 1:
            return pl.ds(all_ - few, few), pl.ds(0, few)
        return pl.ds(0, few), pl.ds(all_ + few, few)

    def p_rows(dy):
        return pl.ds(0, by) if dy == 0 else pl.ds(by, tall)

    def side(dx):
        return 0 if dx == 1 else 1

    def copies_a(d):
        dx, dy, dz = d
        k = code(*d)
        out = [remote(e_out, e_in.at[code(-dx, -dy, -dz)], send_e.at[k], recv_e.at[k], d)]
        if dz != 0:
            slot = code(-dx, -dy, -dz)
            rows = p_rows(dy)
            out.append(
                remote(
                    p_out.at[rows], p_in.at[slot, rows], send_a.at[k, 0], recv_a.at[k, 0], d
                )
            )
        elif dy != 0:
            src, dst = pair_part(dx)
            out.append(
                remote(
                    h_out.at[side(dy), :, src],
                    h_in.at[side(dy), :, dst],
                    send_a.at[k, 0],
                    recv_a.at[k, 0],
                    d,
                )
            )
        else:
            src = x_part(dx)
            for f, ref in enumerate((rhs_ref, cond_ref)):
                out.append(
                    remote(
                        ref.at[src],
                        x_in.at[side(dx), f],
                        send_a.at[k, f],
                        recv_a.at[k, f],
                        d,
                    )
                )
        return out

    def copies_b(d):
        dx, dy, dz = d
        k = code(*d)
        if dz != 0:
            slot = code(-dx, -dy, -dz)
            rows = p_rows(dy)
            return [
                remote(p2_out.at[rows], p2_in.at[slot, rows], send_b.at[k], recv_b.at[k], d)
            ]
        if dy != 0:
            src, dst = pair_part(dx)
            return [
                remote(
                    h2_out.at[side(dy), src], h2_in.at[side(dy), dst], send_b.at[k], recv_b.at[k], d
                )
            ]
        src = x_part(dx)
        return [remote(av_out.at[src], x2_in.at[side(dx)], send_b.at[k], recv_b.at[k], d)]

    def start_all(copies):
        for d in DIRS:

            @pl.when(inside(d))
            def _():
                for c in copies(d):
                    c.start()

    def wait_all(copies):
        for d in DIRS:
            @pl.when(inside(tuple(-a for a in d)))
            def _():
                for c in copies(d):
                    c.wait_recv()

    def wait_sent(copies):
        for d in DIRS:

            @pl.when(inside(d))
            def _():
                for c in copies(d):
                    c.wait_send()

    start_all(copies_a)

    loads[2].wait()
    L = factor_ref[...].astype(f32)
    ri = lax.broadcasted_iota(jnp.int32, (n, n), 0)
    ci = lax.broadcasted_iota(jnp.int32, (n, n), 1)
    eye = ri == ci
    X = jnp.where(eye, 1.0 / jnp.where(eye, L, 1.0), 0.0)
    s = 1
    while s < n:
        pick = (ri // (2 * s) == ci // (2 * s)) & (ri % (2 * s) >= s) & (ci % (2 * s) < s)
        low = jnp.where(pick, L, 0.0)
        X = X - jnp.dot(
            X,
            jnp.dot(low, X, precision=HIGH, preferred_element_type=f32),
            precision=HIGH,
            preferred_element_type=f32,
        )
        s *= 2
    W = lax.dot_general(
        X, X, (((0,), (0,)), ((), ())), precision=HIGH, preferred_element_type=f32
    )

    rowe = lax.broadcasted_iota(jnp.int32, (ey, bz), 0)
    low_lanes = (lane % group) < HALO

    def merge_h(h, x, *at):
        low, high = h[(0,) + at + (x // 2,)], h[(1,) + at + (x // 2,)]
        if x % 2 == 0:
            return jnp.where(row8 < HALO, high, pltpu.roll(low, HALO, 0))
        return jnp.where(row8 < HALO, pltpu.roll(high, HALO, 0), low)

    def merge_p(p):
        merged = []
        for dx in (-1, 0, 1):

            def from_z(dy):
                return jnp.where(
                    low_lanes, p[code(dx, dy, 1)], p[code(dx, dy, -1)]
                ), jnp.where(low_lanes, p[code(dx, dy, -1)], p[code(dx, dy, 1)])

            mid = from_z(0)[1]
            up = from_z(1)[1]
            down = from_z(-1)[1]
            merged.append(
                jnp.where(rowe < by, mid, jnp.where(rowe < by + HALO, up, down))
            )
        return merged

    def where_from(x):
        if x < HALO:
            return 0, bx - HALO + x
        if x < HALO + bx:
            return 1, x - HALO
        return 2, x - HALO - bx

    def unpack(merged, x, f):
        which, slab = where_from(x)
        at = f * bx + slab
        return pltpu.roll(merged[which], (bz - HALO - group * at) % bz, 1)

    wait_all(copies_a)

    merged = merge_p(p_in)
    limits = []
    for dx in (-1, 0, 1):
        sides = []
        for dz in (0, 1, -1):

            def limit(dy):
                if (dx, dy, dz) == (0, 0, 0):
                    return e_out[...]
                return e_in[code(dx, dy, dz)]

            sides.append(
                jnp.where(rowe < by, limit(0), jnp.where(rowe < by + HALO, limit(1), limit(-1)))
            )
        limits.append((sides[0], jnp.where(lane < half, sides[1], sides[2])))
    flags, flags1 = [], []
    lane_f = lane.astype(f32)
    even_f = (lane - lane % 2).astype(f32)
    for a, b in limits:
        flags.append(
            jnp.concatenate([(lane_f < a).astype(f32), (lane_f < b).astype(f32)], axis=1)
        )
        flags1.append(
            jnp.concatenate([(even_f < a).astype(f32), (even_f < b).astype(f32)], axis=1)
        )
    for x in range(ex):
        which, _ = where_from(x)
        FL[x] = flags[which]
        for f, (ref, field) in enumerate(((rhs_ref, R), (cond_ref, C))):
            if which == 1:
                core = ref[x - HALO]
            elif which == 0:
                core = x_in[0, f, x]
            else:
                core = x_in[1, f, x - HALO - bx]
            a = jnp.concatenate([core, merge_h(h_in, x, f)], axis=0)
            whole = jnp.concatenate([a, unpack(merged, x, f)], axis=1)
            field[x] = whole * flags[which] if f == 0 else whole

    wide_lane = lax.broadcasted_iota(jnp.int32, (ey, ez), 1)
    wide_row = lax.broadcasted_iota(jnp.int32, (ey, ez), 0)
    odd_lane = wide_lane % 2 == 1
    odd_row = wide_row % 2 == 1

    def up_y(v, k=1):
        return pltpu.roll(v, k, 0)

    def dn_y(v, k=1):
        return pltpu.roll(v, ey - k, 0)

    def up_z(v, k=1):
        return pltpu.roll(v, k, 1)

    def dn_z(v, k=1):
        return pltpu.roll(v, ez - k, 1)

    def pool_yz(v):
        v = v + jnp.where(odd_row, up_y(v), dn_y(v))
        return v + jnp.where(odd_lane, up_z(v), dn_z(v))

    for x in range(ex):
        c = C[x]
        if x > 0:
            FX[x] = 0.5 * (C[x - 1] + c)
        FY[x] = 0.5 * (c + up_y(c))
        FZ[x] = 0.5 * (c + up_z(c))
    for x in range(1, ex - 1):
        fy, fz = FY[x], FZ[x]
        total = FX[x] + FX[x + 1] + fy + dn_y(fy) + fz + dn_z(fz)
        fl = FL[x]
        INV[x] = OMEGA * fl / (total + 1.0 - fl)
    for q in range(ex // 2):
        C1[q] = pool_yz(C[2 * q] + C[2 * q + 1]) * 0.125
    for q in range(1, ex // 2 - 1):
        c = C1[q]
        total = 3.0 * c + 0.5 * (
            C1[q - 1] + C1[q + 1] + up_y(c, 2) + dn_y(c, 2) + up_z(c, 2) + dn_z(c, 2)
        )
        fl = flags1[where_from(2 * q)[0]]
        IC[q] = OMEGA * fl / (4.0 * total + 1.0 - fl)

    def apply(src, x):
        v = src[x]
        gx = FX[x] * (v - src[x - 1]) + FX[x + 1] * (v - src[x + 1])
        gy = FY[x] * (v - up_y(v))
        gz = FZ[x] * (v - up_z(v))
        return FL[x] * (gx + (gy - dn_y(gy)) + (gz - dn_z(gz)))

    def core(v):
        return v[:by, :bz]

    def cycle():
        for x in range(1, ex - 1):
            FIRST[x] = INV[x] * R[x]
        for q in range(1, ex // 2 - 1):
            a, b = 2 * q, 2 * q + 1
            gap = (R[a] - apply(FIRST, a)) + (R[b] - apply(FIRST, b))
            below = IC[q] * pool_yz(gap)
            SEC[a] = FIRST[a] + FL[a] * below
            SEC[b] = FIRST[b] + FL[b] * below
        for x in range(3, ex - 3):
            V[x] = SEC[x] + INV[x] * (R[x] - apply(SEC, x))

    def total(v):
        return jnp.sum(v, axis=(0, 1), keepdims=True)

    width = gath.shape[-1]
    col = lax.broadcasted_iota(jnp.int32, (1, width), 1)

    def spread(row_ref, g, base):
        everyone(lambda device: remote_row(row_ref, g, base, device).start())

    def remote_row(row_ref, g, base, device):
        return pltpu.make_async_remote_copy(
            src_ref=row_ref,
            dst_ref=g.at[me],
            send_sem=send_g.at[base],
            recv_sem=recv_g.at[base],
            device_id=device,
            device_id_type=MESH,
        )

    def collect(g, base):
        part = g.at[pl.ds(0, n - 1)]
        pltpu.make_async_copy(part, part, recv_g.at[base]).wait()
        pltpu.make_async_copy(part, part, send_g.at[base]).wait()

    cells = bx * by * bz

    cycle()
    sums = [jnp.zeros((by, bz), f32) for _ in range(4)]
    slabs = []
    for x in range(bx):
        e = x + HALO
        av = core(apply(V, e))
        v, r = core(V[e]), core(R[e])
        av_out[x] = av
        slabs.append((av, edge_tile(av)))
        sums = [sums[0] + r, sums[1] + r * v, sums[2] + v * av, sums[3] + av]
    pack_pairs(
        (h2_out.at[0], h2_out.at[1]),
        [v[:tall] for v, _ in slabs],
        [v[by - tall :] for v, _ in slabs],
    )
    p2_out[...] = pack(slabs)
    start_all(copies_b)

    acc = jnp.zeros((by, bz), f32)
    for x in range(HALO, HALO + bx):
        acc = acc + core(apply(FL, x))
    faces = []
    for dx, x, near in ((-1, HALO, HALO - 1), (1, HALO + bx, HALO + bx - 1)):
        other = FL[x] if dx == 1 else FL[near]
        mine = FL[near] if dx == 1 else FL[x]
        faces.append(((dx, 0, 0), total(core(FX[x] * mine * other))))
    first_row = wide_row[:by, :bz] == 0
    last_row = wide_row[:by, :bz] == by - 1
    first_lane = wide_lane[:by, :bz] == 0
    last_lane = wide_lane[:by, :bz] == bz - 1
    cy = jnp.zeros((ey, ez), f32)
    cz = jnp.zeros((ey, ez), f32)
    for x in range(HALO, HALO + bx):
        fl = FL[x]
        cy = cy + FY[x] * fl * up_y(fl)
        cz = cz + FZ[x] * fl * up_z(fl)
    cy_hi, cz_hi = core(dn_y(cy)), core(dn_z(cz))
    faces.append(((0, -1, 0), total(jnp.where(first_row, core(cy), 0.0))))
    faces.append(((0, 1, 0), total(jnp.where(last_row, cy_hi, 0.0))))
    faces.append(((0, 0, -1), total(jnp.where(first_lane, core(cz), 0.0))))
    faces.append(((0, 0, 1), total(jnp.where(last_lane, cz_hi, 0.0))))
    diagonal = total(acc)
    row = jnp.zeros((1, width), f32)
    for (dx, dy, dz), g in faces:
        diagonal = diagonal + g
        other = ((ix + dx) * ngy + iy + dy) * ngz + iz + dz
        row = row - jnp.where(col == bz + other, g, 0.0)
    row = row + jnp.where(col == bz + me, diagonal, 0.0)
    for k, part in enumerate(sums):
        row = jnp.where(col == k, total(part), row)
    row_out[...] = row
    gath[pl.ds(me, 1)] = row[None]
    spread(row_out, gath, 0)
    collect(gath, 0)

    def column(g, k):
        return g[:, 0, k : k + 1]

    def solve(means_col):
        y_row = jnp.sum(W * means_col, axis=0, keepdims=True)
        y_col = jnp.sum(jnp.where(eye, y_row, 0.0), axis=1, keepdims=True)
        return y_row, y_col

    ycol_id = lax.broadcasted_iota(jnp.int32, (ey, n), 1)
    yrow_id = lax.broadcasted_iota(jnp.int32, (ey, n), 0)
    dy_id = jnp.where(yrow_id < by, 0, jnp.where(yrow_id < by + HALO, 1, -1))

    def make_table(y_row):
        for dx in (-1, 0, 1):
            cols = []
            for dz in (0, 1, -1):
                where_at = ((ix + dx) * ngy + iy + dy_id) * ngz + iz + dz
                cols.append(
                    jnp.sum(jnp.where(ycol_id == where_at, y_row, 0.0), axis=1, keepdims=True)
                )
            YT[dx + 1] = jnp.concatenate(
                [
                    jnp.broadcast_to(cols[0], (ey, bz)),
                    jnp.where(lane < half, cols[1], cols[2]),
                ],
                axis=1,
            )

    coupling = gath[:, 0, bz : bz + n]
    m0 = column(gath, 0)
    y_row, y_col = solve(m0 * (1.0 / cells))
    rz = total(column(gath, 1)) + total(m0 * y_col)
    dad = (
        total(column(gath, 2))
        + 2.0 * total(column(gath, 3) * y_col)
        + total(coupling * y_col * y_row)
    )
    alpha = rz / dad
    make_table(y_row)
    for x in range(ex):
        U[x] = FL[x] * YT[where_from(x)[0]]

    wait_all(copies_b)
    merged = merge_p(p2_in)
    for x in range(1, ex - 1):
        which, _ = where_from(x)
        au = apply(U, x)
        if which == 1:
            mid = av_out[x - HALO]
        elif which == 0:
            mid = x2_in[0, x]
        else:
            mid = x2_in[1, x - HALO - bx]
        a = jnp.concatenate([mid, merge_h(h2_in, x)], axis=0)
        ad = jnp.concatenate([a, unpack(merged, x, 0)], axis=1) + au
        R[x] = R[x] - alpha * ad
        if which == 1:
            AD0[x - HALO] = core(ad)
            D0[x - HALO] = core(V[x]) + core(U[x])

    cycle()
    sums = [jnp.zeros((by, bz), f32) for _ in range(6)]
    for x in range(bx):
        e = x + HALO
        av = core(apply(V, e))
        v, r, ad0 = core(V[e]), core(R[e]), AD0[x]
        AV1[x] = av
        sums = [
            sums[0] + r,
            sums[1] + r * v,
            sums[2] + v * av,
            sums[3] + av,
            sums[4] + v * ad0,
            sums[5] + ad0,
        ]
    row = jnp.zeros((1, bz), f32)
    for k, part in enumerate(sums):
        row = jnp.where(col[:, :bz] == k, total(part), row)
    row2_out[...] = row
    gath2[pl.ds(me, 1)] = row[None]
    spread(row2_out, gath2, 1)
    collect(gath2, 1)
    m1 = column(gath2, 0)
    y_row, y_col = solve(m1 * (1.0 / cells))
    new = total(column(gath2, 1)) + total(m1 * y_col)
    beta = new / rz
    dad1 = (
        total(column(gath2, 2))
        + 2.0 * total(column(gath2, 3) * y_col)
        + total(coupling * y_col * y_row)
        + 2.0 * beta * (total(column(gath2, 4)) + total(column(gath2, 5) * y_col))
        + beta * beta * dad
    )
    alpha1 = new / dad1
    make_table(y_row)
    for x in range(HALO - 1, HALO + bx + 1):
        U[x] = FL[x] * YT[where_from(x)[0]]
    for x in range(bx):
        e = x + HALO
        d1 = core(V[e]) + core(U[e]) + beta * D0[x]
        ad1 = AV1[x] + core(apply(U, e)) + beta * AD0[x]
        sol_ref[x] = alpha * D0[x] + alpha1 * d1
        res_ref[x] = core(R[e]) - alpha1 * ad1
    wait_sent(copies_a)
    wait_sent(copies_b)


def solution(mesh):
    counts = (mesh.shape["gx"], mesh.shape["gy"], mesh.shape["gz"])
    n = counts[0] * counts[1] * counts[2]

    def on_device(right_side, conductance, extents, coarse_factor):
        f32 = jnp.float32
        bx, by, bz = right_side.shape
        ex, ey, ez = bx + 2 * HALO, by + 2 * HALO, 2 * bz
        tall = 2 * HALO
        width = bz + -(-n // 128) * 128
        vm = lambda *shape: pltpu.VMEM(shape, f32)
        field = vm(ex, ey, ez)
        dma = pltpu.SemaphoreType.DMA
        scratch = [
            vm(bx, by, bz),
            vm(bx, by, bz),
            pltpu.VMEM(coarse_factor.shape, coarse_factor.dtype),
            vm(2, 2, bx // 2, tall, bz),
            vm(ey, bz),
            vm(1, bz),
            vm(2, 2, HALO, by, bz),
            vm(2, 2, ex // 2, tall, bz),
            vm(27, ey, bz),
            vm(27, 1, bz),
            vm(bx, by, bz),
            vm(2, bx // 2, tall, bz),
            vm(ey, bz),
            vm(2, HALO, by, bz),
            vm(2, ex // 2, tall, bz),
            vm(27, ey, bz),
            vm(1, width),
            vm(1, bz),
            vm(n, 1, width),
            vm(n, 1, bz),
            field,
            field,
            field,
            field,
            field,
            field,
            field,
            vm(ex // 2, ey, ez),
            vm(ex // 2, ey, ez),
            field,
            field,
            field,
            field,
            vm(3, ey, ez),
            vm(bx, by, bz),
            vm(bx, by, bz),
            vm(bx, by, bz),
            dma((27, 2)),
            dma((27, 2)),
            dma((27,)),
            dma((27,)),
            dma((27,)),
            dma((27,)),
            dma((2,)),
            dma((2,)),
            dma((3,)),
        ]
        block = jax.ShapeDtypeStruct((bx, by, bz), f32)
        whole = pl.BlockSpec(memory_space=pltpu.VMEM)
        outer = pl.BlockSpec(memory_space=pltpu.HBM)
        return pl.pallas_call(
            functools.partial(kernel, counts),
            out_shape=(block, block),
            in_specs=[outer, outer, pl.BlockSpec(memory_space=pltpu.SMEM), outer],
            out_specs=(whole, whole),
            scratch_shapes=scratch,
            compiler_params=pltpu.CompilerParams(
                collective_id=0, has_side_effects=True, vmem_limit_bytes=67043328
            ),
        )(right_side, conductance, extents, coarse_factor)

    in_specs = (P("gx", "gy", "gz"), P("gx", "gy", "gz"), P("gx", "gy", "gz"), P())
    out_specs = (P("gx", "gy", "gz"), P("gx", "gy", "gz"))
    return jax.shard_map(
        on_device, mesh=mesh, in_specs=in_specs, out_specs=out_specs, check_vma=False
    )
```

```python
import functools

import jax
import jax.numpy as jnp
from jax import lax
from jax.experimental import pallas as pl
from jax.experimental.pallas import tpu as pltpu
from jax.sharding import PartitionSpec as P

OMEGA = 0.8
HALO = 4
MESH = pl.DeviceIdType.MESH
HIGH = lax.Precision.HIGHEST
DIRS = [
    (dx, dy, dz)
    for dx in (-1, 0, 1)
    for dy in (-1, 0, 1)
    for dz in (-1, 0, 1)
    if (dx, dy, dz) != (0, 0, 0)
]
DIRS.sort(key=lambda d: -sum(abs(a) for a in d))


def code(dx, dy, dz):
    return (dx + 1) * 9 + (dy + 1) * 3 + dz + 1


def kernel(
    counts,
    rhs_hbm,
    cond_hbm,
    ext_ref,
    factor_hbm,
    sol_ref,
    res_ref,
    rhs_ref,
    cond_ref,
    factor_ref,
    h_out,
    p_out,
    e_out,
    x_in,
    h_in,
    p_in,
    e_in,
    av_out,
    h2_out,
    p2_out,
    x2_in,
    h2_in,
    p2_in,
    row_out,
    row2_out,
    gath,
    gath2,
    R,
    C,
    FL,
    FX,
    FY,
    FZ,
    INV,
    C1,
    IC,
    FIRST,
    SEC,
    V,
    U,
    YT,
    D0,
    AD0,
    AV1,
    send_a,
    recv_a,
    send_e,
    recv_e,
    send_b,
    recv_b,
    send_g,
    recv_g,
    load_sem,
):
    ngx, ngy, ngz = counts
    n = ngx * ngy * ngz
    ix, iy, iz = lax.axis_index("gx"), lax.axis_index("gy"), lax.axis_index("gz")
    me = (ix * ngy + iy) * ngz + iz
    bx, by, bz = rhs_ref.shape
    ex, ey, ez = bx + 2 * HALO, by + 2 * HALO, 2 * bz
    group = 2 * HALO
    half = bz // 2
    f32 = jnp.float32

    loads = [
        pltpu.make_async_copy(src, dst, load_sem.at[k])
        for k, (src, dst) in enumerate(
            ((rhs_hbm, rhs_ref), (cond_hbm, cond_ref), (factor_hbm, factor_ref))
        )
    ]
    for load in loads:
        load.start()

    def turned(at, step, count):
        moved = at + step
        return jnp.where(moved >= count, moved - count, moved)

    def everyone(act):
        if n <= 64:
            xs = [turned(ix, t, ngx) for t in range(ngx)]
            ys = [turned(iy, t, ngy) for t in range(ngy)]
            zs = [turned(iz, t, ngz) for t in range(ngz)]
            steps = [(a, b, c) for a in range(ngx) for b in range(ngy) for c in range(ngz)]
            steps.sort(
                key=lambda t: -sum(min(a, m - a) for a, m in zip(t, (ngx, ngy, ngz)))
            )
            for a, b, c in steps[:-1]:
                act((xs[a], ys[b], zs[c]))
        else:

            def one(t, carry):
                flat = (me + t) % n
                act((flat // (ngy * ngz), (flat // ngz) % ngy, flat % ngz))
                return carry

            lax.fori_loop(1, n, one, 0)

    for buf in (x_in, h_in, p_in, e_in, x2_in, h2_in, p2_in):
        buf[...] = jnp.zeros(buf.shape, f32)

    barrier = pltpu.get_barrier_semaphore()
    everyone(
        lambda device: pl.semaphore_signal(
            barrier, inc=1, device_id=device, device_id_type=MESH
        )
    )

    lane = lax.broadcasted_iota(jnp.int32, (ey, bz), 1)
    row8 = lax.broadcasted_iota(jnp.int32, (2 * HALO, bz), 0)

    def edge_tile(slab):
        return jnp.where(row8 < HALO, slab[: 2 * HALO], slab[by - 2 * HALO :])

    def pack_pairs(out, lows, highs):
        for p in range(len(lows) // 2):
            out[0][p] = jnp.where(
                row8 < HALO, pltpu.roll(highs[2 * p], HALO, 0), highs[2 * p + 1]
            )
            out[1][p] = jnp.where(
                row8 < HALO, lows[2 * p], pltpu.roll(lows[2 * p + 1], HALO, 0)
            )

    def pack(slabs):
        packed = jnp.zeros((ey, bz), f32)
        for at, (slab, tile) in enumerate(slabs):
            full = jnp.concatenate([slab, tile], axis=0)
            moved = pltpu.roll(full, (HALO + group * at) % bz, 1)
            packed = jnp.where(lane // group == at, moved, packed)
        return packed

    for load in loads[:2]:
        load.wait()
    tall = 2 * HALO
    slabs = []
    for f, ref in enumerate((rhs_ref, cond_ref)):
        fields = [ref[x] for x in range(bx)]
        pack_pairs(
            (h_out.at[0, f], h_out.at[1, f]),
            [v[:tall] for v in fields],
            [v[by - tall :] for v in fields],
        )
        slabs.extend((v, edge_tile(v)) for v in fields)
    p_out[...] = pack(slabs)
    own_limit = ext_ref[0, 0, 0]
    e_out[...] = jnp.full((1, bz), own_limit.astype(f32), f32)

    pl.semaphore_wait(barrier, n - 1)

    def inside(d):
        dx, dy, dz = d
        ok = None
        for at, step, count in ((ix, dx, ngx), (iy, dy, ngy), (iz, dz, ngz)):
            if step == 0:
                continue
            here = (at + step >= 0) & (at + step < count)
            ok = here if ok is None else ok & here
        return ok

    def target(d):
        return (ix + d[0], iy + d[1], iz + d[2])

    def remote(src, dst, send, recv, d):
        return pltpu.make_async_remote_copy(
            src_ref=src,
            dst_ref=dst,
            send_sem=send,
            recv_sem=recv,
            device_id=target(d),
            device_id_type=MESH,
        )

    def x_part(dx):
        return pl.ds(bx - HALO, HALO) if dx == 1 else pl.ds(0, HALO)

    def pair_part(dx):
        few, all_ = HALO // 2, bx // 2
        if dx == 0:
            return pl.ds(0, all_), pl.ds(few, all_)
        if dx == 1:
            return pl.ds(all_ - few, few), pl.ds(0, few)
        return pl.ds(0, few), pl.ds(all_ + few, few)

    def p_rows(dy):
        return pl.ds(0, by) if dy == 0 else pl.ds(by, tall)

    def side(dx):
        return 0 if dx == 1 else 1

    def copies_a(d):
        dx, dy, dz = d
        k = code(*d)
        out = [remote(e_out, e_in.at[code(-dx, -dy, -dz)], send_e.at[k], recv_e.at[k], d)]
        if dz != 0:
            slot = code(-dx, -dy, -dz)
            rows = p_rows(dy)
            out.append(
                remote(
                    p_out.at[rows], p_in.at[slot, rows], send_a.at[k, 0], recv_a.at[k, 0], d
                )
            )
        elif dy != 0:
            src, dst = pair_part(dx)
            out.append(
                remote(
                    h_out.at[side(dy), :, src],
                    h_in.at[side(dy), :, dst],
                    send_a.at[k, 0],
                    recv_a.at[k, 0],
                    d,
                )
            )
        else:
            src = x_part(dx)
            for f, ref in enumerate((rhs_ref, cond_ref)):
                out.append(
                    remote(
                        ref.at[src],
                        x_in.at[side(dx), f],
                        send_a.at[k, f],
                        recv_a.at[k, f],
                        d,
                    )
                )
        return out

    def copies_b(d):
        dx, dy, dz = d
        k = code(*d)
        if dz != 0:
            slot = code(-dx, -dy, -dz)
            rows = p_rows(dy)
            return [
                remote(p2_out.at[rows], p2_in.at[slot, rows], send_b.at[k], recv_b.at[k], d)
            ]
        if dy != 0:
            src, dst = pair_part(dx)
            return [
                remote(
                    h2_out.at[side(dy), src], h2_in.at[side(dy), dst], send_b.at[k], recv_b.at[k], d
                )
            ]
        src = x_part(dx)
        return [remote(av_out.at[src], x2_in.at[side(dx)], send_b.at[k], recv_b.at[k], d)]

    def start_all(copies):
        for d in DIRS:

            @pl.when(inside(d))
            def _():
                for c in copies(d):
                    c.start()

    def wait_all(copies):
        for d in DIRS:
            @pl.when(inside(tuple(-a for a in d)))
            def _():
                for c in copies(d):
                    c.wait_recv()

    def wait_sent(copies):
        for d in DIRS:

            @pl.when(inside(d))
            def _():
                for c in copies(d):
                    c.wait_send()

    start_all(copies_a)

    loads[2].wait()
    L = factor_ref[...].astype(f32)
    ri = lax.broadcasted_iota(jnp.int32, (n, n), 0)
    ci = lax.broadcasted_iota(jnp.int32, (n, n), 1)
    eye = ri == ci
    X = jnp.where(eye, 1.0 / jnp.where(eye, L, 1.0), 0.0)
    s = 1
    while s < n:
        pick = (ri // (2 * s) == ci // (2 * s)) & (ri % (2 * s) >= s) & (ci % (2 * s) < s)
        low = jnp.where(pick, L, 0.0)
        X = X - jnp.dot(
            X,
            jnp.dot(low, X, precision=HIGH, preferred_element_type=f32),
            precision=HIGH,
            preferred_element_type=f32,
        )
        s *= 2
    W = lax.dot_general(
        X, X, (((0,), (0,)), ((), ())), precision=HIGH, preferred_element_type=f32
    )

    rowe = lax.broadcasted_iota(jnp.int32, (ey, bz), 0)
    low_lanes = (lane % group) < HALO

    def merge_h(h, x, *at):
        low, high = h[(0,) + at + (x // 2,)], h[(1,) + at + (x // 2,)]
        if x % 2 == 0:
            return jnp.where(row8 < HALO, high, pltpu.roll(low, HALO, 0))
        return jnp.where(row8 < HALO, pltpu.roll(high, HALO, 0), low)

    def merge_p(p):
        merged = []
        for dx in (-1, 0, 1):

            def from_z(dy):
                return jnp.where(
                    low_lanes, p[code(dx, dy, 1)], p[code(dx, dy, -1)]
                ), jnp.where(low_lanes, p[code(dx, dy, -1)], p[code(dx, dy, 1)])

            mid = from_z(0)[1]
            up = from_z(1)[1]
            down = from_z(-1)[1]
            merged.append(
                jnp.where(rowe < by, mid, jnp.where(rowe < by + HALO, up, down))
            )
        return merged

    def where_from(x):
        if x < HALO:
            return 0, bx - HALO + x
        if x < HALO + bx:
            return 1, x - HALO
        return 2, x - HALO - bx

    def unpack(merged, x, f):
        which, slab = where_from(x)
        at = f * bx + slab
        return pltpu.roll(merged[which], (bz - HALO - group * at) % bz, 1)

    wait_all(copies_a)

    merged = merge_p(p_in)
    limits = []
    for dx in (-1, 0, 1):
        sides = []
        for dz in (0, 1, -1):

            def limit(dy):
                if (dx, dy, dz) == (0, 0, 0):
                    return e_out[...]
                return e_in[code(dx, dy, dz)]

            sides.append(
                jnp.where(rowe < by, limit(0), jnp.where(rowe < by + HALO, limit(1), limit(-1)))
            )
        limits.append((sides[0], jnp.where(lane < half, sides[1], sides[2])))
    flags, flags1 = [], []
    lane_f = lane.astype(f32)
    even_f = (lane - lane % 2).astype(f32)
    for a, b in limits:
        flags.append(
            jnp.concatenate([(lane_f < a).astype(f32), (lane_f < b).astype(f32)], axis=1)
        )
        flags1.append(
            jnp.concatenate([(even_f < a).astype(f32), (even_f < b).astype(f32)], axis=1)
        )
    for x in range(ex):
        which, _ = where_from(x)
        FL[x] = flags[which]
        for f, (ref, field) in enumerate(((rhs_ref, R), (cond_ref, C))):
            if which == 1:
                core = ref[x - HALO]
            elif which == 0:
                core = x_in[0, f, x]
            else:
                core = x_in[1, f, x - HALO - bx]
            a = jnp.concatenate([core, merge_h(h_in, x, f)], axis=0)
            whole = jnp.concatenate([a, unpack(merged, x, f)], axis=1)
            field[x] = whole * flags[which] if f == 0 else whole

    wide_lane = lax.broadcasted_iota(jnp.int32, (ey, ez), 1)
    wide_row = lax.broadcasted_iota(jnp.int32, (ey, ez), 0)
    odd_lane = wide_lane % 2 == 1
    odd_row = wide_row % 2 == 1

    def up_y(v, k=1):
        return pltpu.roll(v, k, 0)

    def dn_y(v, k=1):
        return pltpu.roll(v, ey - k, 0)

    def up_z(v, k=1):
        return pltpu.roll(v, k, 1)

    def dn_z(v, k=1):
        return pltpu.roll(v, ez - k, 1)

    def pool_yz(v):
        v = v + jnp.where(odd_row, up_y(v), dn_y(v))
        return v + jnp.where(odd_lane, up_z(v), dn_z(v))

    for x in range(ex):
        c = C[x]
        if x > 0:
            FX[x] = 0.5 * (C[x - 1] + c)
        FY[x] = 0.5 * (c + up_y(c))
        FZ[x] = 0.5 * (c + up_z(c))
    for x in range(1, ex - 1):
        fy, fz = FY[x], FZ[x]
        total = FX[x] + FX[x + 1] + fy + dn_y(fy) + fz + dn_z(fz)
        fl = FL[x]
        INV[x] = OMEGA * fl / (total + 1.0 - fl)
    for q in range(ex // 2):
        C1[q] = pool_yz(C[2 * q] + C[2 * q + 1]) * 0.125
    for q in range(1, ex // 2 - 1):
        c = C1[q]
        total = 3.0 * c + 0.5 * (
            C1[q - 1] + C1[q + 1] + up_y(c, 2) + dn_y(c, 2) + up_z(c, 2) + dn_z(c, 2)
        )
        fl = flags1[where_from(2 * q)[0]]
        IC[q] = OMEGA * fl / (4.0 * total + 1.0 - fl)

    def apply(src, x):
        v = src[x]
        gx = FX[x] * (v - src[x - 1]) + FX[x + 1] * (v - src[x + 1])
        gy = FY[x] * (v - up_y(v))
        gz = FZ[x] * (v - up_z(v))
        return FL[x] * (gx + (gy - dn_y(gy)) + (gz - dn_z(gz)))

    def core(v):
        return v[:by, :bz]

    def cycle():
        for x in range(1, ex - 1):
            FIRST[x] = INV[x] * R[x]
        for q in range(1, ex // 2 - 1):
            a, b = 2 * q, 2 * q + 1
            gap = (R[a] - apply(FIRST, a)) + (R[b] - apply(FIRST, b))
            below = IC[q] * pool_yz(gap)
            SEC[a] = FIRST[a] + FL[a] * below
            SEC[b] = FIRST[b] + FL[b] * below
        for x in range(3, ex - 3):
            V[x] = SEC[x] + INV[x] * (R[x] - apply(SEC, x))

    def total(v):
        return jnp.sum(v, axis=(0, 1), keepdims=True)

    width = gath.shape[-1]
    col = lax.broadcasted_iota(jnp.int32, (1, width), 1)

    def spread(row_ref, g, base):
        everyone(lambda device: remote_row(row_ref, g, base, device).start())

    def remote_row(row_ref, g, base, device):
        return pltpu.make_async_remote_copy(
            src_ref=row_ref,
            dst_ref=g.at[me],
            send_sem=send_g.at[base],
            recv_sem=recv_g.at[base],
            device_id=device,
            device_id_type=MESH,
        )

    def collect(g, base):
        part = g.at[pl.ds(0, n - 1)]
        pltpu.make_async_copy(part, part, recv_g.at[base]).wait()
        pltpu.make_async_copy(part, part, send_g.at[base]).wait()

    cells = bx * by * bz

    cycle()
    sums = [jnp.zeros((by, bz), f32) for _ in range(4)]
    slabs = []
    for x in range(bx):
        e = x + HALO
        av = core(apply(V, e))
        v, r = core(V[e]), core(R[e])
        av_out[x] = av
        slabs.append((av, edge_tile(av)))
        sums = [sums[0] + r, sums[1] + r * v, sums[2] + v * av, sums[3] + av]
    pack_pairs(
        (h2_out.at[0], h2_out.at[1]),
        [v[:tall] for v, _ in slabs],
        [v[by - tall :] for v, _ in slabs],
    )
    p2_out[...] = pack(slabs)
    start_all(copies_b)

    acc = jnp.zeros((by, bz), f32)
    for x in range(HALO, HALO + bx):
        acc = acc + core(apply(FL, x))
    faces = []
    for dx, x, near in ((-1, HALO, HALO - 1), (1, HALO + bx, HALO + bx - 1)):
        other = FL[x] if dx == 1 else FL[near]
        mine = FL[near] if dx == 1 else FL[x]
        faces.append(((dx, 0, 0), total(core(FX[x] * mine * other))))
    first_row = wide_row[:by, :bz] == 0
    last_row = wide_row[:by, :bz] == by - 1
    first_lane = wide_lane[:by, :bz] == 0
    last_lane = wide_lane[:by, :bz] == bz - 1
    cy = jnp.zeros((ey, ez), f32)
    cz = jnp.zeros((ey, ez), f32)
    for x in range(HALO, HALO + bx):
        fl = FL[x]
        cy = cy + FY[x] * fl * up_y(fl)
        cz = cz + FZ[x] * fl * up_z(fl)
    cy_hi, cz_hi = core(dn_y(cy)), core(dn_z(cz))
    faces.append(((0, -1, 0), total(jnp.where(first_row, core(cy), 0.0))))
    faces.append(((0, 1, 0), total(jnp.where(last_row, cy_hi, 0.0))))
    faces.append(((0, 0, -1), total(jnp.where(first_lane, core(cz), 0.0))))
    faces.append(((0, 0, 1), total(jnp.where(last_lane, cz_hi, 0.0))))
    diagonal = total(acc)
    row = jnp.zeros((1, width), f32)
    for (dx, dy, dz), g in faces:
        diagonal = diagonal + g
        other = ((ix + dx) * ngy + iy + dy) * ngz + iz + dz
        row = row - jnp.where(col == bz + other, g, 0.0)
    row = row + jnp.where(col == bz + me, diagonal, 0.0)
    for k, part in enumerate(sums):
        row = jnp.where(col == k, total(part), row)
    row_out[...] = row
    gath[pl.ds(me, 1)] = row[None]
    spread(row_out, gath, 0)
    collect(gath, 0)

    def column(g, k):
        return g[:, 0, k : k + 1]

    def solve(means_col):
        y_row = jnp.sum(W * means_col, axis=0, keepdims=True)
        y_col = jnp.sum(jnp.where(eye, y_row, 0.0), axis=1, keepdims=True)
        return y_row, y_col

    ycol_id = lax.broadcasted_iota(jnp.int32, (ey, n), 1)
    yrow_id = lax.broadcasted_iota(jnp.int32, (ey, n), 0)
    dy_id = jnp.where(yrow_id < by, 0, jnp.where(yrow_id < by + HALO, 1, -1))

    def make_table(y_row):
        for dx in (-1, 0, 1):
            cols = []
            for dz in (0, 1, -1):
                where_at = ((ix + dx) * ngy + iy + dy_id) * ngz + iz + dz
                cols.append(
                    jnp.sum(jnp.where(ycol_id == where_at, y_row, 0.0), axis=1, keepdims=True)
                )
            YT[dx + 1] = jnp.concatenate(
                [
                    jnp.broadcast_to(cols[0], (ey, bz)),
                    jnp.where(lane < half, cols[1], cols[2]),
                ],
                axis=1,
            )

    coupling = gath[:, 0, bz : bz + n]
    m0 = column(gath, 0)
    y_row, y_col = solve(m0 * (1.0 / cells))
    rz = total(column(gath, 1)) + total(m0 * y_col)
    dad = (
        total(column(gath, 2))
        + 2.0 * total(column(gath, 3) * y_col)
        + total(coupling * y_col * y_row)
    )
    alpha = rz / dad
    make_table(y_row)
    for x in range(ex):
        U[x] = FL[x] * YT[where_from(x)[0]]

    wait_all(copies_b)
    merged = merge_p(p2_in)
    for x in range(1, ex - 1):
        which, _ = where_from(x)
        au = apply(U, x)
        if which == 1:
            mid = av_out[x - HALO]
        elif which == 0:
            mid = x2_in[0, x]
        else:
            mid = x2_in[1, x - HALO - bx]
        a = jnp.concatenate([mid, merge_h(h2_in, x)], axis=0)
        ad = jnp.concatenate([a, unpack(merged, x, 0)], axis=1) + au
        R[x] = R[x] - alpha * ad
        if which == 1:
            AD0[x - HALO] = core(ad)
            D0[x - HALO] = core(V[x]) + core(U[x])

    cycle()
    sums = [jnp.zeros((by, bz), f32) for _ in range(6)]
    for x in range(bx):
        e = x + HALO
        av = core(apply(V, e))
        v, r, ad0 = core(V[e]), core(R[e]), AD0[x]
        AV1[x] = av
        sums = [
            sums[0] + r,
            sums[1] + r * v,
            sums[2] + v * av,
            sums[3] + av,
            sums[4] + v * ad0,
            sums[5] + ad0,
        ]
    row = jnp.zeros((1, bz), f32)
    for k, part in enumerate(sums):
        row = jnp.where(col[:, :bz] == k, total(part), row)
    row2_out[...] = row
    gath2[pl.ds(me, 1)] = row[None]
    spread(row2_out, gath2, 1)
    collect(gath2, 1)
    m1 = column(gath2, 0)
    y_row, y_col = solve(m1 * (1.0 / cells))
    new = total(column(gath2, 1)) + total(m1 * y_col)
    beta = new / rz
    dad1 = (
        total(column(gath2, 2))
        + 2.0 * total(column(gath2, 3) * y_col)
        + total(coupling * y_col * y_row)
        + 2.0 * beta * (total(column(gath2, 4)) + total(column(gath2, 5) * y_col))
        + beta * beta * dad
    )
    alpha1 = new / dad1
    make_table(y_row)
    for x in range(HALO - 1, HALO + bx + 1):
        U[x] = FL[x] * YT[where_from(x)[0]]
    for x in range(bx):
        e = x + HALO
        d1 = core(V[e]) + core(U[e]) + beta * D0[x]
        ad1 = AV1[x] + core(apply(U, e)) + beta * AD0[x]
        sol_ref[x] = alpha * D0[x] + alpha1 * d1
        res_ref[x] = core(R[e]) - alpha1 * ad1
    wait_sent(copies_a)
    wait_sent(copies_b)


def solution(mesh):
    counts = (mesh.shape["gx"], mesh.shape["gy"], mesh.shape["gz"])
    n = counts[0] * counts[1] * counts[2]

    def on_device(right_side, conductance, extents, coarse_factor):
        f32 = jnp.float32
        bx, by, bz = right_side.shape
        ex, ey, ez = bx + 2 * HALO, by + 2 * HALO, 2 * bz
        tall = 2 * HALO
        width = bz + -(-n // 128) * 128
        vm = lambda *shape: pltpu.VMEM(shape, f32)
        field = vm(ex, ey, ez)
        dma = pltpu.SemaphoreType.DMA
        scratch = [
            vm(bx, by, bz),
            vm(bx, by, bz),
            pltpu.VMEM(coarse_factor.shape, coarse_factor.dtype),
            vm(2, 2, bx // 2, tall, bz),
            vm(ey, bz),
            vm(1, bz),
            vm(2, 2, HALO, by, bz),
            vm(2, 2, ex // 2, tall, bz),
            vm(27, ey, bz),
            vm(27, 1, bz),
            vm(bx, by, bz),
            vm(2, bx // 2, tall, bz),
            vm(ey, bz),
            vm(2, HALO, by, bz),
            vm(2, ex // 2, tall, bz),
            vm(27, ey, bz),
            vm(1, width),
            vm(1, bz),
            vm(n, 1, width),
            vm(n, 1, bz),
            field,
            field,
            field,
            field,
            field,
            field,
            field,
            vm(ex // 2, ey, ez),
            vm(ex // 2, ey, ez),
            field,
            field,
            field,
            field,
            vm(3, ey, ez),
            vm(bx, by, bz),
            vm(bx, by, bz),
            vm(bx, by, bz),
            dma((27, 2)),
            dma((27, 2)),
            dma((27,)),
            dma((27,)),
            dma((27,)),
            dma((27,)),
            dma((2,)),
            dma((2,)),
            dma((3,)),
        ]
        block = vm(bx, by, bz)
        whole = pl.BlockSpec(memory_space=pltpu.VMEM)
        outer = pl.BlockSpec(memory_space=pltpu.HBM)
        return pl.pallas_call(
            functools.partial(kernel, counts),
            out_shape=(block, block),
            in_specs=[outer, outer, pl.BlockSpec(memory_space=pltpu.SMEM), outer],
            out_specs=(whole, whole),
            scratch_shapes=scratch,
            compiler_params=pltpu.CompilerParams(
                collective_id=0, has_side_effects=True, vmem_limit_bytes=60000000
            ),
        )(right_side, conductance, extents, coarse_factor)

    in_specs = (P("gx", "gy", "gz"), P("gx", "gy", "gz"), P("gx", "gy", "gz"), P())
    out_specs = (P("gx", "gy", "gz"), P("gx", "gy", "gz"))
    return jax.shard_map(
        on_device, mesh=mesh, in_specs=in_specs, out_specs=out_specs, check_vma=False
    )
```
